32 devices in a mesh: dp: 8 (over z, y), tensor: 4 (over x, core).
Axes of the slice: x: 2, y: 2, z: 4, core: 2. Of those that a mesh axis runs over, the one named last changes fastest.
Arguments:
- tokens: bfloat16 [16, 1024, 1280], P('dp', 'tensor'), may hold values from -6 to 6
- pic_ids: int32 [16, 1024], P('dp'), may hold values from 0 to 9, as said below
- pos_rows: int32 [16, 1024], P('dp'), may hold values from 0 to 31, as said below
- pos_cols: int32 [16, 1024], P('dp'), may hold values from 0 to 31, as said below
- lengths: int32 [16, 10], P('dp'), may hold values from 0 to 1024, as said below
- ln1_gain: bfloat16 [1280], P(('dp', 'tensor')), may hold values from 0.5 to 1.5
- ln1_bias: bfloat16 [1280], P(('dp', 'tensor')), may hold values from -4 to 4
- qkv_weight: bfloat16 [1280, 3, 1280], P('dp', None, 'tensor'), may hold values from -0.25 to 0.25
- qkv_bias: bfloat16 [3840], P(('dp', 'tensor')), may hold values from -4 to 4
- proj_weight: bfloat16 [1280, 1280], P('tensor', 'dp'), may hold values from -0.3125 to 0.3125
- proj_bias: bfloat16 [1280], P(('dp', 'tensor')), may hold values from -4 to 4
- ln2_gain: bfloat16 [1280], P(('dp', 'tensor')), may hold values from 0.5 to 1.5
- ln2_bias: bfloat16 [1280], P(('dp', 'tensor')), may hold values from -4 to 4
- fc1_weight: bfloat16 [1280, 5120], P('dp', 'tensor'), may hold values from -0.15625 to 0.15625
- fc1_bias: bfloat16 [5120], P(('dp', 'tensor')), may hold values from -6 to 6
- fc2_weight: bfloat16 [5120, 1280], P('tensor', 'dp'), may hold values from -0.078125 to 0.078125
- fc2_bias: bfloat16 [1280], P(('dp', 'tensor')), may hold values from -4 to 4
- cotangent: bfloat16 [16, 1024, 1280], P('dp', 'tensor'), may hold values from -6 to 6
Outputs:
- output: bfloat16 [16, 1024, 1280], P('dp', 'tensor')
- tokens_grad: bfloat16 [16, 1024, 1280], P('dp', 'tensor')
- ln1_gain_grad: float32 [1280], P(('dp', 'tensor'))
- ln1_bias_grad: float32 [1280], P(('dp', 'tensor'))
- qkv_weight_grad: float32 [1280, 3, 1280], P('dp', None, 'tensor')
- qkv_bias_grad: float32 [3840], P(('dp', 'tensor'))
- proj_weight_grad: float32 [1280, 1280], P('tensor', 'dp')
- proj_bias_grad: float32 [1280], P(('dp', 'tensor'))
- ln2_gain_grad: float32 [1280], P(('dp', 'tensor'))
- ln2_bias_grad: float32 [1280], P(('dp', 'tensor'))
- fc1_weight_grad: float32 [1280, 5120], P('dp', 'tensor')
- fc1_bias_grad: float32 [5120], P(('dp', 'tensor'))
- fc2_weight_grad: float32 [5120, 1280], P('tensor', 'dp')
- fc2_bias_grad: float32 [1280], P(('dp', 'tensor'))
The draws below stay inside these ranges and needn't reach their ends.
Inputs may be any that keep to these rules, and one draw needn't show every extreme that they name: `pic_ids`: in each row the used picture slots come first and their patches stand in slot order from position 0; padding slots follow at the row's end and carry the number of the row's last picture. `pos_rows`: each picture's patches are listed by 2 x 2 blocks of its grid, blocks in row order. `pos_cols`: as for pos_rows. A used slot holds the product of two even sides from 10 to 32; unused slots hold 0 and follow the used ones; a row's lengths sum to more than 824 and at most 1024.
All inputs are finite; a program needn't handle non-finite values.
Results may differ from the reference program's by a relative error of at most 0.019.
Values may be sent and summed in bfloat16 or wider, within the bound.
A program may use at most 256 MiB of HBM per device.

```python
import math
import jax
import jax.numpy as jnp
from jax import lax

D = 1280
HEADS = 16
HEAD_DIM = 80
FF = 5120
SEQ = 1024
SIDE_MIN = 10
SIDE_MAX = 32
ROWS = 16


def picture_layout(key):
    smallest = SIDE_MIN * SIDE_MIN
    slot_count = SEQ // smallest
    places = jnp.arange(SEQ, dtype=jnp.int32)
    slot_ids = jnp.arange(slot_count, dtype=jnp.int32)

    def one_row(row_key, row_number):
        reserve_key = jax.random.fold_in(row_key, 100003)
        reserved = jax.random.randint(reserve_key, (), 1, smallest + 1, dtype=jnp.int32)
        reserved = jnp.where(row_number == 0, 0, reserved).astype(jnp.int32)

        def one_slot(remaining, slot_index):
            slot_key = jax.random.fold_in(row_key, slot_index)
            key_height, key_width = jax.random.split(slot_key)
            is_alive = remaining >= smallest
            top_height = jnp.maximum(jnp.minimum(SIDE_MAX, remaining // SIDE_MIN) // 2 * 2, SIDE_MIN)
            height = 2 * jax.random.randint(key_height, (), SIDE_MIN // 2, top_height // 2 + 1, dtype=jnp.int32)
            top_width = jnp.maximum(jnp.minimum(SIDE_MAX, remaining // height) // 2 * 2, SIDE_MIN)
            breadth = 2 * jax.random.randint(key_width, (), SIDE_MIN // 2, top_width // 2 + 1, dtype=jnp.int32)
            forced = (row_number == 0) & (slot_index == 0)
            height = jnp.where(forced, SIDE_MAX, height)
            breadth = jnp.where(forced, SIDE_MAX, breadth)
            tiny_row = row_number == 1
            height = jnp.where(tiny_row, SIDE_MIN, height)
            breadth = jnp.where(tiny_row, SIDE_MIN, breadth)
            size_now = jnp.where(is_alive, height * breadth, 0).astype(jnp.int32)
            breadth = jnp.where(is_alive, breadth, 0).astype(jnp.int32)
            return ((remaining - size_now).astype(jnp.int32), (size_now, breadth))
        leftover, (picture_sizes, breadths) = lax.scan(one_slot, (SEQ - reserved).astype(jnp.int32), slot_ids)
        offsets = jnp.cumsum(picture_sizes) - picture_sizes
        filled_total = jnp.sum(picture_sizes)
        pictures = jnp.sum((picture_sizes > 0).astype(jnp.int32))
        member = ((places[:, None] >= offsets[None, :]) & (places[:, None] < (offsets + picture_sizes)[None, :])).astype(jnp.int32)
        filled = places < filled_total
        picture = jnp.where(filled, jnp.sum(member * slot_ids[None, :], axis=1), pictures - 1)
        inside_index = places - jnp.sum(member * offsets[None, :], axis=1)
        across = jnp.maximum(jnp.sum(member * breadths[None, :], axis=1) // 2, 1)
        block_number = inside_index // 4
        within = inside_index % 4
        row_place = jnp.where(filled, 2 * (block_number // across) + within // 2, 0)
        col_place = jnp.where(filled, 2 * (block_number % across) + within % 2, 0)
        return (picture.astype(jnp.int32), row_place.astype(jnp.int32), col_place.astype(jnp.int32), picture_sizes.astype(jnp.int32))
    row_keys = jax.vmap(lambda row_number: jax.random.fold_in(key, row_number))(jnp.arange(ROWS, dtype=jnp.int32))
    return jax.vmap(one_row)(row_keys, jnp.arange(ROWS, dtype=jnp.int32))


def draw_pic_ids(key, part):
    return picture_layout(key)[0]


def draw_pos_rows(key, part):
    return picture_layout(key)[1]


def draw_pos_cols(key, part):
    return picture_layout(key)[2]


def draw_lengths(key, part):
    return picture_layout(key)[3]


def spiked(array, own_key, source, target, shards_of, factor):
    owner, partner = [(jnp.arange(array.shape[position]) // (array.shape[position] // shards_of)).reshape([-1 if axis == position else 1 for axis in range(array.ndim)]) for position in (source, target)]
    chosen = jax.random.permutation(own_key, shards_of)[partner]
    strong = (owner == chosen) | (owner == (partner + shards_of // 2) % shards_of)
    return jnp.where(strong, factor * array, array)


def level_of(key, dims, cuts, low, high):
    gain = 1.0
    for axis_at, shards_of in cuts:
        heights = jax.random.uniform(jax.random.fold_in(jax.random.fold_in(key, 6), axis_at), (shards_of,), jnp.float32, low / len(cuts), high / len(cuts))
        gain = gain * jnp.repeat(jnp.exp(heights), dims[axis_at] // shards_of).reshape((-1,) + (1,) * (len(dims) - 1 - axis_at))
    return gain


def noise(key, dims, scale, most, pieces=(), kind=jnp.bfloat16):
    values = scale * jax.random.normal(key, dims, jnp.float32)
    if pieces:
        values = values * level_of(key, dims, pieces, -0.22, 0.18)
    return jnp.clip(values, -most, most).astype(kind)


def heavy_noise(key, shape, deviation, bound, cuts, heavy, kind=jnp.bfloat16):
    entries = deviation * jax.random.normal(key, shape, jnp.float32)
    if cuts:
        entries = entries * level_of(key, shape, cuts, -0.22, 0.18)
    return jnp.clip(spiked(entries, jax.random.fold_in(key, 3), *heavy), -bound, bound).astype(kind)


def setup_inputs(seed: int = 0) -> dict:
    key_of = jax.random.split(jax.random.key(seed), 19)
    return {
        "tokens": noise(key_of[0], (ROWS, SEQ, D), 1.0, 6.0, ((0, 8), (1, 4))),
        "pic_ids": draw_pic_ids(jax.random.fold_in(key_of[18], 71), 0),
        "pos_rows": draw_pos_rows(jax.random.fold_in(key_of[18], 71), 0),
        "pos_cols": draw_pos_cols(jax.random.fold_in(key_of[18], 71), 0),
        "lengths": draw_lengths(jax.random.fold_in(key_of[18], 71), 0),
        "ln1_gain": jnp.clip(1.0 + 0.1 * jax.random.normal(key_of[5], (D,), jnp.float32), 0.5, 1.5).astype(jnp.bfloat16),
        "ln1_bias": noise(key_of[6], (D,), 0.3, 4.0, ((0, 32),)),
        "qkv_weight": noise(key_of[7], (D, 3, D), (D // 2) ** -0.5, 0.25, ((0, 8), (2, 4))),
        "qkv_bias": noise(key_of[8], (3 * D,), 0.3, 4.0, ((0, 32),)),
        "proj_weight": noise(key_of[9], (D, D), (D // 4) ** -0.5, 0.3125, ((0, 4), (1, 8))),
        "proj_bias": noise(key_of[10], (D,), 0.3, 4.0, ((0, 32),)),
        "ln2_gain": jnp.clip(1.0 + 0.1 * jax.random.normal(key_of[11], (D,), jnp.float32), 0.5, 1.5).astype(jnp.bfloat16),
        "ln2_bias": noise(key_of[12], (D,), 0.3, 4.0, ((0, 32),)),
        "fc1_weight": noise(key_of[13], (D, FF), D ** -0.5, 0.15625, ((0, 8), (1, 4))),
        "fc1_bias": noise(key_of[14], (FF,), 0.5, 6.0, ((0, 32),)),
        "fc2_weight": noise(key_of[15], (FF, D), FF ** -0.5, 0.078125, ((0, 4), (1, 8))),
        "fc2_bias": noise(key_of[16], (D,), 0.3, 4.0, ((0, 32),)),
        "cotangent": heavy_noise(key_of[17], (ROWS, SEQ, D), 1.0, 6.0, ((0, 8), (1, 4)), (0, 2, 8, 2.0)),
    }


@jax.custom_vjp
def low(v):
    return lax.optimization_barrier(v.astype(jnp.bfloat16)).astype(jnp.float32)

@jax.custom_vjp
def low_back(v):
    return v

def low_keep(v):
    return (low(v), None)

def low_pass(kept, grad):
    return (grad,)

def back_keep(v):
    return (v, None)

def back_low(kept, grad):
    return (low(grad),)
low.defvjp(low_keep, low_pass)
low_back.defvjp(back_keep, back_low)

def layer_norm(values, gain_row, shift_row):
    center = values - lax.optimization_barrier(jnp.mean(values, axis=-1, keepdims=True))
    spread = lax.optimization_barrier(jnp.mean(center * center, axis=-1, keepdims=True))
    return center * lax.rsqrt(spread + 1e-06) * gain_row + shift_row

def rotate_half(values):
    middle = values.shape[-1] // 2
    return jnp.concatenate([-values[..., middle:], values[..., :middle]], axis=-1)

def rotary_tables(row_places, col_places):
    quarter = HEAD_DIM // 4
    freqs_base = 10000.0 ** (-(4.0 * jnp.arange(quarter, dtype=jnp.float32)) / HEAD_DIM)
    angles = jnp.concatenate([row_places.astype(jnp.float32)[:, None] * freqs_base[None, :], col_places.astype(jnp.float32)[:, None] * freqs_base[None, :]], axis=-1)
    angles = jnp.concatenate([angles, angles], axis=-1)[:, None, :]
    return (jnp.cos(angles), jnp.sin(angles))

def rotary_apply(values, cos_table, sin_table):
    return values * cos_table + rotate_half(values) * sin_table

def key_window(row_ids, row_lengths):
    slot_ids = jnp.arange(row_lengths.shape[0], dtype=jnp.int32)
    offsets = jnp.cumsum(row_lengths) - row_lengths
    picked = (row_ids[:, None] == slot_ids[None, :]).astype(jnp.int32)
    window_start = lax.optimization_barrier(jnp.sum(picked * offsets[None, :], axis=1))
    return (window_start, window_start + lax.optimization_barrier(jnp.sum(picked * row_lengths[None, :], axis=1)))

def row_forward(params, row_tokens, row_ids, row_rows, row_cols, row_lengths):
    gain_one, shift_one, w_qkv, b_qkv, w_proj, b_proj, gain_two, shift_two, w_fc1, b_fc1, w_fc2, b_fc2 = params
    highest = lax.Precision.HIGHEST
    row_length = row_tokens.shape[0]
    lowered_one = low(layer_norm(row_tokens, gain_one, shift_one))
    linear = jnp.einsum('sd,dke->ske', lowered_one, w_qkv, precision=highest) + b_qkv.reshape(3, -1)[None]
    linear = low_back(linear)
    split_heads = linear.reshape(row_length, 3, HEADS, HEAD_DIM)
    cos_table, sin_table = rotary_tables(row_rows, row_cols)
    queries = low(rotary_apply(split_heads[:, 0], cos_table, sin_table))
    keys_low = low(rotary_apply(split_heads[:, 1], cos_table, sin_table))
    values_low = low(split_heads[:, 2])
    window_start, window_stop = key_window(row_ids, row_lengths)
    places = jnp.arange(row_length, dtype=jnp.int32)
    inside = (places[None, :] >= window_start[:, None]) & (places[None, :] < window_stop[:, None])
    raw_scores = low_back(jnp.einsum('qhd,khd->hqk', queries, keys_low, precision=highest))
    scores = jnp.where(inside[None], raw_scores * (1.0 / math.sqrt(HEAD_DIM)), -1e+30)
    attend = jax.nn.softmax(scores, axis=-1)
    context = jnp.einsum('hqk,khd->qhd', low(attend), values_low, precision=highest).reshape(row_length, HEADS * HEAD_DIM)
    context = low(low_back(context))
    hidden_state = row_tokens + low_back(jnp.dot(context, w_proj, precision=highest)) + b_proj
    lowered_two = low(layer_norm(hidden_state, gain_two, shift_two))
    upward = low_back(jnp.dot(lowered_two, w_fc1, precision=highest) + b_fc1)
    activated = low(upward * jax.nn.sigmoid(1.702 * upward))
    branch = low_back(jnp.dot(activated, w_fc2, precision=highest)) + b_fc2
    row_pad = (places < jnp.sum(row_lengths)).astype(jnp.float32)
    return row_pad[:, None] * (hidden_state + branch)

def reference(tokens, pic_ids, pos_rows, pos_cols, lengths, ln1_gain, ln1_bias, qkv_weight, qkv_bias, proj_weight, proj_bias, ln2_gain, ln2_bias, fc1_weight, fc1_bias, fc2_weight, fc2_bias, cotangent):
    params = tuple((member.astype(jnp.float32) for member in (ln1_gain, ln1_bias, qkv_weight, qkv_bias, proj_weight, proj_bias, ln2_gain, ln2_bias, fc1_weight, fc1_bias, fc2_weight, fc2_bias)))

    def forward_all(weights, inputs):

        def one_row(packed):
            return row_forward(weights, *packed)
        return lax.map(jax.checkpoint(one_row), (inputs, pic_ids, pos_rows, pos_cols, lengths))
    result, pull_back = jax.vjp(forward_all, params, tokens.astype(jnp.float32))
    weight_grads, token_grad = pull_back(cotangent.astype(jnp.float32))
    return (result.astype(jnp.bfloat16), token_grad.astype(jnp.bfloat16), weight_grads[0], weight_grads[1], weight_grads[2], weight_grads[3], weight_grads[4], weight_grads[5], weight_grads[6], weight_grads[7], weight_grads[8], weight_grads[9], weight_grads[10], weight_grads[11])
```

```python
import functools
import math

import jax
import jax.numpy as jnp
from jax import lax
from jax.sharding import PartitionSpec as P

HEAD_DIM = 80


norm_eps = 1e-06
masked_score = -1e30


def layer_norm(values, gain_row, shift_row):
    center = values - jnp.mean(values, axis=-1, keepdims=True)
    spread = jnp.mean(center * center, axis=-1, keepdims=True)
    scaled = lax.rsqrt(spread + norm_eps)
    normed = center * scaled
    return (normed * gain_row + shift_row, normed, scaled)


def norm_back(grad_rows, normed, scaled, gain_row):
    grad_hat = grad_rows * gain_row
    mean_one = jnp.mean(grad_hat, axis=-1, keepdims=True)
    mean_two = jnp.mean(grad_hat * normed, axis=-1, keepdims=True)
    return scaled * (grad_hat - mean_one - normed * mean_two)


def rotate_half(values):
    middle = values.shape[-1] // 2
    return jnp.concatenate([-values[..., middle:], values[..., :middle]], axis=-1)


def rotary_tables(row_places, col_places, head_size):
    quarter = head_size // 4
    freqs_base = 10000.0 ** (-(4.0 * jnp.arange(quarter, dtype=jnp.float32)) / head_size)
    angles = jnp.concatenate(
        [
            row_places.astype(jnp.float32)[:, None] * freqs_base[None, :],
            col_places.astype(jnp.float32)[:, None] * freqs_base[None, :],
        ],
        axis=-1,
    )
    angles = jnp.concatenate([angles, angles], axis=-1)[:, None, :]
    return (jnp.cos(angles), jnp.sin(angles))


def rotary_apply(values, cos_table, sin_table):
    return values * cos_table + rotate_half(values) * sin_table


def rotary_back(grad_rows, cos_table, sin_table):
    return grad_rows * cos_table - rotate_half(grad_rows * sin_table)


def key_window(row_ids, row_lengths):
    slot_ids = jnp.arange(row_lengths.shape[0], dtype=jnp.int32)
    offsets = jnp.cumsum(row_lengths) - row_lengths
    picked = (row_ids[:, None] == slot_ids[None, :]).astype(jnp.int32)
    window_start = jnp.sum(picked * offsets[None, :], axis=1)
    return (window_start, window_start + jnp.sum(picked * row_lengths[None, :], axis=1))


def flip_pairs(count, step):
    return [(place, place ^ step) for place in range(count)]


def relative_order(count):
    order = [0]
    step = count // 2
    while step >= 1:
        order = order + [place ^ step for place in order]
        step //= 2
    return order


def gather_rows(rows, count):
    step = count // 2
    while step >= 1:
        received = lax.ppermute(rows, "tensor", flip_pairs(count, step))
        rows = jnp.concatenate([rows, received], axis=0)
        step //= 2
    return rows


def scatter_product(product, rows, count):
    half = rows.shape[0] // 2
    sent = product(rows[half:]).astype(jnp.bfloat16)
    received = lax.ppermute(sent, "tensor", flip_pairs(count, 1))
    total = product(rows[:half]) + received.astype(jnp.float32)
    step = 2
    while step < count:
        half = half // 2
        received = lax.ppermute(
            total[half:].astype(jnp.bfloat16), "tensor", flip_pairs(count, step)
        )
        total = total[:half] + received.astype(jnp.float32)
        step *= 2
    return total


def gather_small(vectors, dp_count, tensor_count):
    count = dp_count * tensor_count
    place = lax.axis_index("dp") * tensor_count + lax.axis_index("tensor")
    packed = jnp.concatenate(vectors, axis=0)
    width = packed.shape[0]
    table = lax.dynamic_update_slice_in_dim(
        jnp.zeros((count, width), packed.dtype), packed[None], place, 0
    )
    step = 1
    while step < count:
        table = table + lax.ppermute(table, ("dp", "tensor"), flip_pairs(count, step))
        step *= 2
    parts = []
    offset = 0
    for vector in vectors:
        size = vector.shape[0]
        parts.append(table[:, offset : offset + size].reshape(count * size))
        offset += size
    return parts


def scatter_small(vectors, dp_count, tensor_count):
    count = dp_count * tensor_count
    place = lax.axis_index("dp") * tensor_count + lax.axis_index("tensor")
    table = jnp.concatenate([vector.reshape(count, -1) for vector in vectors], axis=1)
    near = lax.bitwise_xor(jnp.arange(count, dtype=jnp.int32), place.astype(jnp.int32))
    table = jnp.take(table, near, axis=0)
    step = count // 2
    while step >= 1:
        received = lax.ppermute(table[step:], ("dp", "tensor"), flip_pairs(count, step))
        table = table[:step] + received
        step //= 2
    parts = []
    offset = 0
    for vector in vectors:
        size = vector.shape[0] // count
        parts.append(table[0, offset : offset + size])
        offset += size
    return parts


def block_scores(query_block, keys_bf, start_block, stop_block, key_places, score_scale):
    scores = (
        jnp.einsum("qhd,khd->hqk", query_block, keys_bf, preferred_element_type=jnp.float32)
        * score_scale
    )
    inside = (key_places[None, :] >= start_block[:, None]) & (
        key_places[None, :] < stop_block[:, None]
    )
    return jnp.where(inside[None], scores, masked_score)


def attend_forward(linear, tables, score_scale):
    cos_table, sin_table, start_all, stop_all, key_places = tables
    row_length = linear.shape[0]
    block_rows = min(512, row_length)
    queries_bf = rotary_apply(linear[:, 0], cos_table, sin_table).astype(jnp.bfloat16)
    keys_bf = rotary_apply(linear[:, 1], cos_table, sin_table).astype(jnp.bfloat16)
    values_bf = linear[:, 2].astype(jnp.bfloat16)
    context_blocks = []
    logsum_blocks = []
    for lower in range(0, row_length, block_rows):
        upper = lower + block_rows
        scores = block_scores(
            queries_bf[lower:upper],
            keys_bf,
            start_all[lower:upper],
            stop_all[lower:upper],
            key_places,
            score_scale,
        )
        highest = jnp.max(scores, axis=-1, keepdims=True)
        shifted = jnp.exp(scores - highest)
        totals = jnp.sum(shifted, axis=-1, keepdims=True)
        attend = shifted / totals
        logsum_blocks.append(highest + jnp.log(totals))
        context_blocks.append(
            jnp.einsum(
                "hqk,khd->qhd",
                attend.astype(jnp.bfloat16),
                values_bf,
                preferred_element_type=jnp.float32,
            )
        )
    context_bf = jnp.concatenate(context_blocks, axis=0).astype(jnp.bfloat16)
    return context_bf, (queries_bf, keys_bf, values_bf, logsum_blocks)


def attend_back(kept, grad_context, tables, score_scale):
    cos_table, sin_table, start_all, stop_all, key_places = tables
    queries_bf, keys_bf, values_bf, logsum_blocks = kept
    row_length, head_count, _ = queries_bf.shape
    block_rows = min(512, row_length)
    grad_keys = jnp.zeros((row_length, head_count, HEAD_DIM), jnp.float32)
    grad_values = jnp.zeros((row_length, head_count, HEAD_DIM), jnp.float32)
    query_grad_blocks = []
    for block_index, lower in enumerate(range(0, row_length, block_rows)):
        upper = lower + block_rows
        scores = block_scores(
            queries_bf[lower:upper],
            keys_bf,
            start_all[lower:upper],
            stop_all[lower:upper],
            key_places,
            score_scale,
        )
        attend = jnp.exp(scores - logsum_blocks[block_index])
        context_grad = grad_context[lower:upper]
        grad_values = grad_values + jnp.einsum(
            "hqk,qhd->khd",
            attend.astype(jnp.bfloat16),
            context_grad,
            preferred_element_type=jnp.float32,
        )
        attend_grad = jnp.einsum(
            "qhd,khd->hqk", context_grad, values_bf, preferred_element_type=jnp.float32
        )
        row_inner = jnp.sum(attend * attend_grad, axis=-1, keepdims=True)
        score_grad = (attend * (attend_grad - row_inner) * score_scale).astype(jnp.bfloat16)
        query_grad_blocks.append(
            jnp.einsum("hqk,khd->qhd", score_grad, keys_bf, preferred_element_type=jnp.float32)
        )
        grad_keys = grad_keys + jnp.einsum(
            "hqk,qhd->khd",
            score_grad,
            queries_bf[lower:upper],
            preferred_element_type=jnp.float32,
        )
    grad_queries = jnp.concatenate(query_grad_blocks, axis=0)
    return jnp.stack(
        [
            rotary_back(grad_queries, cos_table, sin_table),
            rotary_back(grad_keys, cos_table, sin_table),
            grad_values,
        ],
        axis=1,
    ).astype(jnp.bfloat16)


def dot_nn(left, right):
    return jnp.dot(left, right, preferred_element_type=jnp.float32)


def dot_nt(left, right):
    return jnp.einsum("sk,nk->sn", left, right, preferred_element_type=jnp.float32)


def dot_tn(left, right):
    return jnp.einsum("sm,sn->mn", left, right, preferred_element_type=jnp.float32)


def on_device(
    dp_count,
    tensor_count,
    tokens,
    pic_ids,
    pos_rows,
    pos_cols,
    lengths,
    ln1_gain,
    ln1_bias,
    qkv_weight,
    qkv_bias,
    proj_weight,
    proj_bias,
    ln2_gain,
    ln2_bias,
    fc1_weight,
    fc1_bias,
    fc2_weight,
    fc2_bias,
    cotangent,
):
    row_total = tokens.shape[0]
    local_rows = tokens.shape[1]
    model_width = tokens.shape[2]
    row_length = pic_ids.shape[1]
    head_width = qkv_weight.shape[2]
    hidden_width = fc1_weight.shape[1]
    head_count = head_width // HEAD_DIM
    score_scale = 1.0 / math.sqrt(HEAD_DIM)
    tensor_place = lax.axis_index("tensor")
    f32 = jnp.float32
    bf16 = jnp.bfloat16
    order = jnp.array(relative_order(tensor_count), jnp.int32)
    block_ids = lax.bitwise_xor(order, tensor_place.astype(jnp.int32))
    all_places = (
        block_ids[:, None] * local_rows + jnp.arange(local_rows, dtype=jnp.int32)[None, :]
    ).reshape(row_length)

    def near_order(values):
        return jnp.take(values.reshape(tensor_count, local_rows), block_ids, axis=0).reshape(
            row_length
        )

    local_places = all_places[:local_rows]
    vectors = gather_small(
        (ln1_gain, ln1_bias, qkv_bias, proj_bias, ln2_gain, ln2_bias, fc1_bias, fc2_bias),
        dp_count,
        tensor_count,
    )
    gain_one, shift_one, qkv_shift, proj_shift, gain_two, shift_two, fc1_shift, fc2_shift = [
        vector_part.astype(f32) for vector_part in vectors
    ]
    qkv_local_shift = lax.dynamic_slice_in_dim(
        qkv_shift.reshape(3, model_width), tensor_place * head_width, head_width, 1
    ).reshape(3 * head_width)
    fc1_local_shift = lax.dynamic_slice_in_dim(
        fc1_shift, tensor_place * hidden_width, hidden_width, 0
    )
    w_qkv = lax.all_gather(qkv_weight, "dp", axis=0, tiled=True)
    w_proj = lax.all_gather(proj_weight, "dp", axis=1, tiled=True)
    w_fc1 = lax.all_gather(fc1_weight, "dp", axis=0, tiled=True)
    w_fc2 = lax.all_gather(fc2_weight, "dp", axis=1, tiled=True)
    w_qkv_flat = w_qkv.reshape(model_width, 3 * head_width)

    outputs = []
    saved = []
    for row in range(row_total):
        tokens_row = tokens[row].astype(f32)
        start_all, stop_all = key_window(near_order(pic_ids[row]), lengths[row])
        cos_table, sin_table = rotary_tables(
            near_order(pos_rows[row]), near_order(pos_cols[row]), HEAD_DIM
        )
        tables = (cos_table, sin_table, start_all, stop_all, all_places)
        pad_rows = (local_places < jnp.sum(lengths[row])).astype(f32)[:, None]
        grad_out = pad_rows * cotangent[row].astype(f32)
        grad_branch = gather_rows(grad_out.astype(bf16), tensor_count)
        normed_one, hat_one, scale_one = layer_norm(tokens_row, gain_one, shift_one)
        lowered_one = gather_rows(normed_one.astype(bf16), tensor_count)
        linear = dot_nn(lowered_one, w_qkv_flat) + qkv_local_shift
        linear = linear.reshape(row_length, 3, head_count, HEAD_DIM)
        context_bf, kept = attend_forward(linear, tables, score_scale)
        context_bf = context_bf.reshape(row_length, head_width)
        attn_branch = scatter_product(
            lambda part: dot_nn(part, w_proj), context_bf, tensor_count
        )
        hidden_row = tokens_row + attn_branch + proj_shift
        normed_two, hat_two, scale_two = layer_norm(hidden_row, gain_two, shift_two)
        lowered_two = gather_rows(normed_two.astype(bf16), tensor_count)
        upward = dot_nn(lowered_two, w_fc1) + fc1_local_shift
        activated = (upward * jax.nn.sigmoid(1.702 * upward)).astype(bf16)
        branch = scatter_product(lambda part: dot_nn(part, w_fc2), activated, tensor_count)
        outputs.append((pad_rows * (hidden_row + branch + fc2_shift)).astype(bf16))
        saved.append(
            (
                tables,
                grad_out,
                grad_branch,
                hat_one,
                scale_one,
                lowered_one,
                context_bf,
                kept,
                hat_two,
                scale_two,
                lowered_two,
                upward,
                activated,
            )
        )

    token_grads = []
    totals = None
    for row in range(row_total):
        (
            tables,
            grad_out,
            grad_branch,
            hat_one,
            scale_one,
            lowered_one,
            context_bf,
            kept,
            hat_two,
            scale_two,
            lowered_two,
            upward,
            activated,
        ) = saved[row]
        micro_fc2 = dot_tn(activated, grad_branch)
        sigmoid_up = jax.nn.sigmoid(1.702 * upward)
        grad_up = (
            dot_nt(grad_branch, w_fc2)
            * (sigmoid_up + 1.702 * upward * sigmoid_up * (1.0 - sigmoid_up))
        ).astype(bf16)
        micro_fc1 = dot_tn(lowered_two, grad_up)
        grad_normed_two = scatter_product(
            lambda part: dot_nt(part, w_fc1), grad_up, tensor_count
        )
        grad_hidden = grad_out + norm_back(grad_normed_two, hat_two, scale_two, gain_two)
        grad_attn = gather_rows(grad_hidden.astype(bf16), tensor_count)
        micro_proj = dot_tn(context_bf, grad_attn)
        grad_context = (
            dot_nt(grad_attn, w_proj).astype(bf16).reshape(row_length, head_count, HEAD_DIM)
        )
        grad_linear = attend_back(kept, grad_context, tables, score_scale).reshape(
            row_length, 3 * head_width
        )
        micro_qkv = dot_tn(lowered_one, grad_linear)
        grad_normed_one = scatter_product(
            lambda part: dot_nt(part, w_qkv_flat), grad_linear, tensor_count
        )
        token_grads.append(
            (grad_hidden + norm_back(grad_normed_one, hat_one, scale_one, gain_one)).astype(bf16)
        )
        parts = (
            jnp.sum(grad_normed_one * hat_one, axis=0),
            jnp.sum(grad_normed_one, axis=0),
            jnp.sum(grad_linear.astype(f32), axis=0),
            jnp.sum(grad_hidden, axis=0),
            jnp.sum(grad_normed_two * hat_two, axis=0),
            jnp.sum(grad_normed_two, axis=0),
            jnp.sum(grad_up.astype(f32), axis=0),
            jnp.sum(grad_out, axis=0),
            micro_qkv,
            micro_proj,
            micro_fc1,
            micro_fc2,
        )
        totals = parts if totals is None else tuple(a + b for a, b in zip(totals, parts))

    grad_fc2 = lax.psum_scatter(
        totals[11].astype(bf16), "dp", scatter_dimension=1, tiled=True
    ).astype(f32)
    grad_fc1 = lax.psum_scatter(
        totals[10].astype(bf16), "dp", scatter_dimension=0, tiled=True
    ).astype(f32)
    grad_proj = lax.psum_scatter(
        totals[9].astype(bf16), "dp", scatter_dimension=1, tiled=True
    ).astype(f32)
    grad_qkv = lax.psum_scatter(
        totals[8].reshape(model_width, 3, head_width).astype(bf16),
        "dp",
        scatter_dimension=0,
        tiled=True,
    ).astype(f32)
    qkv_full_grad = lax.dynamic_update_slice_in_dim(
        jnp.zeros((3, model_width), f32),
        totals[2].reshape(3, head_width),
        tensor_place * head_width,
        1,
    ).reshape(3 * model_width)
    fc1_full_grad = lax.dynamic_update_slice_in_dim(
        jnp.zeros((fc1_shift.shape[0],), f32), totals[6], tensor_place * hidden_width, 0
    )
    small_out = scatter_small(
        (
            totals[0],
            totals[1],
            qkv_full_grad,
            totals[3],
            totals[4],
            totals[5],
            fc1_full_grad,
            totals[7],
        ),
        dp_count,
        tensor_count,
    )
    return (
        jnp.stack(outputs, axis=0),
        jnp.stack(token_grads, axis=0),
        small_out[0],
        small_out[1],
        grad_qkv,
        small_out[2],
        grad_proj,
        small_out[3],
        small_out[4],
        small_out[5],
        grad_fc1,
        small_out[6],
        grad_fc2,
        small_out[7],
    )


def solution(mesh):
    placed = (
        P("dp", "tensor", None),
        P("dp", None),
        P("dp", None),
        P("dp", None),
        P("dp", None),
        P(("dp", "tensor")),
        P(("dp", "tensor")),
        P("dp", None, "tensor"),
        P(("dp", "tensor")),
        P("tensor", "dp"),
        P(("dp", "tensor")),
        P(("dp", "tensor")),
        P(("dp", "tensor")),
        P("dp", "tensor"),
        P(("dp", "tensor")),
        P("tensor", "dp"),
        P(("dp", "tensor")),
        P("dp", "tensor", None),
    )
    return jax.shard_map(
        functools.partial(on_device, mesh.shape["dp"], mesh.shape["tensor"]),
        mesh=mesh,
        in_specs=placed,
        out_specs=(
            P("dp", "tensor", None),
            P("dp", "tensor", None),
            P(("dp", "tensor")),
            P(("dp", "tensor")),
            P("dp", None, "tensor"),
            P(("dp", "tensor")),
            P("tensor", "dp"),
            P(("dp", "tensor")),
            P(("dp", "tensor")),
            P(("dp", "tensor")),
            P("dp", "tensor"),
            P(("dp", "tensor")),
            P("tensor", "dp"),
            P(("dp", "tensor")),
        ),
        check_vma=False,
    )
```

```python
import functools
import math

import jax
import jax.numpy as jnp
from jax import lax
from jax.experimental import pallas as pl
from jax.experimental.pallas import tpu as pltpu
from jax.sharding import PartitionSpec as P

HEAD_DIM = 80


norm_eps = 1e-06


def layer_norm(values, gain_row, shift_row):
    center = values - jnp.mean(values, axis=-1, keepdims=True)
    spread = jnp.mean(center * center, axis=-1, keepdims=True)
    scaled = lax.rsqrt(spread + norm_eps)
    normed = center * scaled
    return (normed * gain_row + shift_row, normed, scaled)


def norm_back(grad_rows, normed, scaled, gain_row):
    grad_hat = grad_rows * gain_row
    mean_one = jnp.mean(grad_hat, axis=-1, keepdims=True)
    mean_two = jnp.mean(grad_hat * normed, axis=-1, keepdims=True)
    return scaled * (grad_hat - mean_one - normed * mean_two)


def flip_pairs(count, step):
    return [(place, place ^ step) for place in range(count)]


def relative_order(count):
    order = [0]
    step = count // 2
    while step >= 1:
        order = order + [place ^ step for place in order]
        step //= 2
    return order


def gather_rows(rows, count):
    step = count // 2
    while step >= 1:
        received = lax.ppermute(rows, "tensor", flip_pairs(count, step))
        rows = jnp.concatenate([rows, received], axis=0)
        step //= 2
    return rows


def scatter_product(product, rows, count):
    half = rows.shape[0] // 2
    sent = product(rows[half:]).astype(jnp.bfloat16)
    received = lax.ppermute(sent, "tensor", flip_pairs(count, 1))
    total = product(rows[:half]) + received.astype(jnp.float32)
    step = 2
    while step < count:
        half = half // 2
        received = lax.ppermute(
            total[half:].astype(jnp.bfloat16), "tensor", flip_pairs(count, step)
        )
        total = total[:half] + received.astype(jnp.float32)
        step *= 2
    return total


def gather_small(vectors, dp_count, tensor_count):
    count = dp_count * tensor_count
    place = lax.axis_index("dp") * tensor_count + lax.axis_index("tensor")
    packed = jnp.concatenate(vectors, axis=0)
    width = packed.shape[0]
    table = lax.dynamic_update_slice_in_dim(
        jnp.zeros((count, width), packed.dtype), packed[None], place, 0
    )
    step = 1
    while step < count:
        table = table + lax.ppermute(table, ("dp", "tensor"), flip_pairs(count, step))
        step *= 2
    parts = []
    offset = 0
    for vector in vectors:
        size = vector.shape[0]
        parts.append(table[:, offset : offset + size].reshape(count * size))
        offset += size
    return parts


def scatter_small(vectors, dp_count, tensor_count):
    count = dp_count * tensor_count
    place = lax.axis_index("dp") * tensor_count + lax.axis_index("tensor")
    table = jnp.concatenate([vector.reshape(count, -1) for vector in vectors], axis=1)
    near = lax.bitwise_xor(jnp.arange(count, dtype=jnp.int32), place.astype(jnp.int32))
    table = jnp.take(table, near, axis=0)
    step = count // 2
    while step >= 1:
        received = lax.ppermute(table[step:], ("dp", "tensor"), flip_pairs(count, step))
        table = table[:step] + received
        step //= 2
    parts = []
    offset = 0
    for vector in vectors:
        size = vector.shape[0] // count
        parts.append(table[0, offset : offset + size])
        offset += size
    return parts


LANES = 128
away = 2.0 ** 66
log2_e = 1.4426950408889634


def fold_lanes(values):
    quarter_turn = HEAD_DIM // 2
    return (
        pltpu.roll(values, LANES - quarter_turn, 1),
        pltpu.roll(values, quarter_turn, 1),
    )


def nt_product(left, right):
    return lax.dot_general(
        left, right, (((1,), (1,)), ((), ())), preferred_element_type=jnp.float32
    )


def attend_forward_kernel(
    block_rows,
    score_scale,
    lin_q_ref,
    lin_k_ref,
    lin_v_ref,
    cos_ref,
    sin_low_ref,
    sin_high_ref,
    query_slot_ref,
    key_slot_ref,
    query_ref,
    key_ref,
    value_ref,
    context_ref,
    stat_ref,
):
    row_length = lin_q_ref.shape[0]

    def turned(values, slots):
        low, high = fold_lanes(values)
        return (
            values * cos_ref[...] + low * sin_low_ref[...] + high * sin_high_ref[...] + slots
        ).astype(jnp.bfloat16)

    query_ref[...] = turned(lin_q_ref[...], query_slot_ref[...])
    keys = turned(lin_k_ref[...], key_slot_ref[...])
    key_ref[...] = keys
    values = lin_v_ref[...].astype(jnp.bfloat16)
    value_ref[...] = values
    values_t = values.T
    for lower in range(0, row_length, block_rows):
        block = slice(lower, lower + block_rows)
        scores = nt_product(keys, query_ref[block, :])
        highest = jnp.max(scores, axis=0, keepdims=True)
        shifted = jnp.exp2((scores - highest) * (score_scale * log2_e))
        inverse = 1.0 / jnp.sum(shifted, axis=0, keepdims=True)
        attend = (shifted * inverse).astype(jnp.bfloat16)
        context_t = jnp.dot(values_t, attend, preferred_element_type=jnp.float32)
        context_ref[block, :] = context_t.T.astype(jnp.bfloat16)
        stat_ref[0, 0:1, block] = highest
        stat_ref[0, 1:2, block] = inverse


def attend_back_kernel(
    block_rows,
    score_scale,
    query_ref,
    key_ref,
    value_ref,
    grad_ref,
    stat_ref,
    cos_ref,
    sin_low_ref,
    sin_high_ref,
    grad_linear_ref,
    key_sum_ref,
    value_sum_ref,
):
    row_length = query_ref.shape[0]
    head = pl.program_id(0)
    heads = pl.num_programs(0)
    keys = key_ref[...]
    keys_t = keys.T
    values = value_ref[...]

    def columns(kind):
        return pl.ds(pl.multiple_of((kind * heads + head) * LANES, LANES), LANES)

    def unturned(grads, block):
        low, high = fold_lanes(grads)
        return (
            grads * cos_ref[block, :] - low * sin_low_ref[block, :] - high * sin_high_ref[block, :]
        ).astype(jnp.bfloat16)

    for lower in range(0, row_length, block_rows):
        block = slice(lower, lower + block_rows)
        queries = query_ref[block, :]
        grads = grad_ref[block, :]
        scores = nt_product(keys, queries)
        attend = (
            jnp.exp2((scores - stat_ref[0, 0:1, block]) * (score_scale * log2_e))
            * stat_ref[0, 1:2, block]
        )
        value_part = jnp.dot(
            attend.astype(jnp.bfloat16), grads, preferred_element_type=jnp.float32
        )
        attend_grad = nt_product(values, grads)
        inner = jnp.sum(attend * attend_grad, axis=0, keepdims=True)
        score_grad = (attend * (attend_grad - inner) * score_scale).astype(jnp.bfloat16)
        key_part = jnp.dot(score_grad, queries, preferred_element_type=jnp.float32)
        query_t = jnp.dot(keys_t, score_grad, preferred_element_type=jnp.float32)
        grad_linear_ref[block, columns(0)] = unturned(query_t.T, block)
        if lower == 0:
            key_sum_ref[...] = key_part
            value_sum_ref[...] = value_part
        else:
            key_sum_ref[...] += key_part
            value_sum_ref[...] += value_part
    grad_linear_ref[:, columns(1)] = unturned(key_sum_ref[...], slice(None))
    grad_linear_ref[:, columns(2)] = value_sum_ref[...].astype(jnp.bfloat16)


def head_spec(row_length, shift):
    return pl.BlockSpec((row_length, LANES), lambda head: (0, head + shift))


def whole_spec(shape):
    return pl.BlockSpec(shape, lambda head: (0,) * len(shape))


def attend_forward(linear, tables, head_count, score_scale):
    row_length = linear.shape[0]
    block_rows = min(256, row_length)
    cos_table, sin_low, sin_high, query_slots, key_slots = tables
    table = whole_spec((row_length, LANES))
    headed = jax.ShapeDtypeStruct((row_length, head_count * LANES), jnp.bfloat16)
    area = head_count * row_length * row_length
    queries, keys, values, context, stats = pl.pallas_call(
        functools.partial(attend_forward_kernel, block_rows, score_scale),
        grid=(head_count,),
        in_specs=[
            head_spec(row_length, 0),
            head_spec(row_length, head_count),
            head_spec(row_length, 2 * head_count),
        ]
        + [table] * 5,
        out_specs=[head_spec(row_length, 0)] * 4
        + [pl.BlockSpec((1, 2, row_length), lambda head: (head, 0, 0))],
        out_shape=[headed] * 4
        + [jax.ShapeDtypeStruct((head_count, 2, row_length), jnp.float32)],
        cost_estimate=pl.CostEstimate(
            flops=4 * area * LANES,
            bytes_accessed=20 * row_length * head_count * LANES,
            transcendentals=area,
        ),
        name="attend_forward",
    )(linear, linear, linear, cos_table, sin_low, sin_high, query_slots, key_slots)
    return context, (queries, keys, values, stats)


def attend_back(kept, grad_context, tables, head_count, score_scale):
    queries, keys, values, stats = kept
    row_length = queries.shape[0]
    block_rows = min(256, row_length)
    cos_table, sin_low, sin_high = tables[:3]
    table = whole_spec((row_length, LANES))
    area = head_count * row_length * row_length
    return pl.pallas_call(
        functools.partial(attend_back_kernel, block_rows, score_scale),
        grid=(head_count,),
        in_specs=[head_spec(row_length, 0)] * 4
        + [pl.BlockSpec((1, 2, row_length), lambda head: (head, 0, 0))]
        + [table] * 3,
        out_specs=whole_spec((row_length, 3 * head_count * LANES)),
        out_shape=jax.ShapeDtypeStruct((row_length, 3 * head_count * LANES), jnp.bfloat16),
        scratch_shapes=[
            pltpu.VMEM((row_length, LANES), jnp.float32),
            pltpu.VMEM((row_length, LANES), jnp.float32),
        ],
        cost_estimate=pl.CostEstimate(
            flops=10 * area * LANES,
            bytes_accessed=14 * row_length * head_count * LANES,
            transcendentals=area,
        ),
        name="attend_back",
    )(queries, keys, values, grad_context, stats, cos_table, sin_low, sin_high)


def head_tables(row_places, col_places, row_ids, row_lengths, key_places):
    quarter = HEAD_DIM // 4
    half = HEAD_DIM // 2
    slots = row_lengths.shape[0]
    freqs_base = 10000.0 ** (-(4.0 * jnp.arange(quarter, dtype=jnp.float32)) / HEAD_DIM)
    angles = jnp.concatenate(
        [
            row_places.astype(jnp.float32)[:, None] * freqs_base[None, :],
            col_places.astype(jnp.float32)[:, None] * freqs_base[None, :],
        ],
        axis=-1,
    )
    cosine = jnp.cos(angles)
    sine = jnp.sin(angles)

    def lanes(values, before):
        return jnp.pad(values, ((0, 0), (before, LANES - before - values.shape[1])))

    same = row_ids[:, None] == jnp.arange(slots, dtype=jnp.int32)[None, :]
    filled = (key_places < jnp.sum(row_lengths))[:, None]
    low_sine = lanes(sine, 0)
    high_sine = lanes(sine, half)
    return (
        lanes(jnp.concatenate([cosine, cosine], axis=-1), 0),
        -low_sine,
        high_sine,
        lanes(same.astype(jnp.float32), HEAD_DIM),
        lanes(jnp.where(same & filled, 0.0, -away), HEAD_DIM),
    )


def dot_nn(left, right):
    return jnp.dot(left, right, preferred_element_type=jnp.float32)


def dot_nt(left, right):
    return jnp.einsum("sk,nk->sn", left, right, preferred_element_type=jnp.float32)


def dot_tn(left, right):
    return jnp.einsum("sm,sn->mn", left, right, preferred_element_type=jnp.float32)


def on_device(
    dp_count,
    tensor_count,
    tokens,
    pic_ids,
    pos_rows,
    pos_cols,
    lengths,
    ln1_gain,
    ln1_bias,
    qkv_weight,
    qkv_bias,
    proj_weight,
    proj_bias,
    ln2_gain,
    ln2_bias,
    fc1_weight,
    fc1_bias,
    fc2_weight,
    fc2_bias,
    cotangent,
):
    row_total = tokens.shape[0]
    local_rows = tokens.shape[1]
    model_width = tokens.shape[2]
    row_length = pic_ids.shape[1]
    head_width = qkv_weight.shape[2]
    hidden_width = fc1_weight.shape[1]
    head_count = head_width // HEAD_DIM
    score_scale = 1.0 / math.sqrt(HEAD_DIM)
    tensor_place = lax.axis_index("tensor")
    f32 = jnp.float32
    bf16 = jnp.bfloat16
    order = jnp.array(relative_order(tensor_count), jnp.int32)
    block_ids = lax.bitwise_xor(order, tensor_place.astype(jnp.int32))
    all_places = (
        block_ids[:, None] * local_rows + jnp.arange(local_rows, dtype=jnp.int32)[None, :]
    ).reshape(row_length)

    def near_order(values):
        return jnp.take(values.reshape(tensor_count, local_rows), block_ids, axis=0).reshape(
            row_length
        )

    local_places = all_places[:local_rows]
    vectors = gather_small(
        (ln1_gain, ln1_bias, qkv_bias, proj_bias, ln2_gain, ln2_bias, fc1_bias, fc2_bias),
        dp_count,
        tensor_count,
    )
    gain_one, shift_one, qkv_shift, proj_shift, gain_two, shift_two, fc1_shift, fc2_shift = [
        vector_part.astype(f32) for vector_part in vectors
    ]
    qkv_local_shift = lax.dynamic_slice_in_dim(
        qkv_shift.reshape(3, model_width), tensor_place * head_width, head_width, 1
    ).reshape(3 * head_width)
    fc1_local_shift = lax.dynamic_slice_in_dim(
        fc1_shift, tensor_place * hidden_width, hidden_width, 0
    )
    w_qkv = lax.all_gather(qkv_weight, "dp", axis=0, tiled=True)
    w_proj = lax.all_gather(proj_weight, "dp", axis=1, tiled=True)
    w_fc1 = lax.all_gather(fc1_weight, "dp", axis=0, tiled=True)
    w_fc2 = lax.all_gather(fc2_weight, "dp", axis=1, tiled=True)
    spare = LANES - HEAD_DIM
    w_qkv_flat = jnp.pad(
        w_qkv.reshape(model_width, 3 * head_count, HEAD_DIM), ((0, 0), (0, 0), (0, spare))
    ).reshape(model_width, 3 * head_count * LANES)
    w_proj = jnp.pad(
        w_proj.reshape(head_count, HEAD_DIM, model_width), ((0, 0), (0, spare), (0, 0))
    ).reshape(head_count * LANES, model_width)
    qkv_local_shift = jnp.pad(
        qkv_local_shift.reshape(3 * head_count, HEAD_DIM), ((0, 0), (0, spare))
    ).reshape(3 * head_count * LANES)

    outputs = []
    saved = []
    for row in range(row_total):
        tokens_row = tokens[row].astype(f32)
        tables = head_tables(
            near_order(pos_rows[row]),
            near_order(pos_cols[row]),
            near_order(pic_ids[row]),
            lengths[row],
            all_places,
        )
        pad_rows = (local_places < jnp.sum(lengths[row])).astype(f32)[:, None]
        grad_out = pad_rows * cotangent[row].astype(f32)
        grad_branch = gather_rows(grad_out.astype(bf16), tensor_count)
        normed_one, hat_one, scale_one = layer_norm(tokens_row, gain_one, shift_one)
        lowered_one = gather_rows(normed_one.astype(bf16), tensor_count)
        linear = dot_nn(lowered_one, w_qkv_flat) + qkv_local_shift
        context_bf, kept = attend_forward(linear, tables, head_count, score_scale)
        attn_branch = scatter_product(
            lambda part: dot_nn(part, w_proj), context_bf, tensor_count
        )
        hidden_row = tokens_row + attn_branch + proj_shift
        normed_two, hat_two, scale_two = layer_norm(hidden_row, gain_two, shift_two)
        lowered_two = gather_rows(normed_two.astype(bf16), tensor_count)
        upward = dot_nn(lowered_two, w_fc1) + fc1_local_shift
        activated = (upward * jax.nn.sigmoid(1.702 * upward)).astype(bf16)
        branch = scatter_product(lambda part: dot_nn(part, w_fc2), activated, tensor_count)
        outputs.append((pad_rows * (hidden_row + branch + fc2_shift)).astype(bf16))
        saved.append(
            (
                tables,
                grad_out,
                grad_branch,
                hat_one,
                scale_one,
                lowered_one,
                context_bf,
                kept,
                hat_two,
                scale_two,
                lowered_two,
                upward,
                activated,
            )
        )

    token_grads = []
    totals = None
    for row in range(row_total):
        (
            tables,
            grad_out,
            grad_branch,
            hat_one,
            scale_one,
            lowered_one,
            context_bf,
            kept,
            hat_two,
            scale_two,
            lowered_two,
            upward,
            activated,
        ) = saved[row]
        micro_fc2 = dot_tn(activated, grad_branch)
        sigmoid_up = jax.nn.sigmoid(1.702 * upward)
        grad_up = (
            dot_nt(grad_branch, w_fc2)
            * (sigmoid_up + 1.702 * upward * sigmoid_up * (1.0 - sigmoid_up))
        ).astype(bf16)
        micro_fc1 = dot_tn(lowered_two, grad_up)
        grad_normed_two = scatter_product(
            lambda part: dot_nt(part, w_fc1), grad_up, tensor_count
        )
        grad_hidden = grad_out + norm_back(grad_normed_two, hat_two, scale_two, gain_two)
        grad_attn = gather_rows(grad_hidden.astype(bf16), tensor_count)
        micro_proj = dot_tn(context_bf, grad_attn)
        grad_context = dot_nt(grad_attn, w_proj).astype(bf16)
        grad_linear = attend_back(kept, grad_context, tables, head_count, score_scale)
        micro_qkv = dot_tn(lowered_one, grad_linear)
        grad_normed_one = scatter_product(
            lambda part: dot_nt(part, w_qkv_flat), grad_linear, tensor_count
        )
        token_grads.append(
            (grad_hidden + norm_back(grad_normed_one, hat_one, scale_one, gain_one)).astype(bf16)
        )
        parts = (
            jnp.sum(grad_normed_one * hat_one, axis=0),
            jnp.sum(grad_normed_one, axis=0),
            jnp.sum(grad_linear.astype(f32), axis=0),
            jnp.sum(grad_hidden, axis=0),
            jnp.sum(grad_normed_two * hat_two, axis=0),
            jnp.sum(grad_normed_two, axis=0),
            jnp.sum(grad_up.astype(f32), axis=0),
            jnp.sum(grad_out, axis=0),
            micro_qkv,
            micro_proj,
            micro_fc1,
            micro_fc2,
        )
        totals = parts if totals is None else tuple(a + b for a, b in zip(totals, parts))

    grad_fc2 = lax.psum_scatter(
        totals[11].astype(bf16), "dp", scatter_dimension=1, tiled=True
    ).astype(f32)
    grad_fc1 = lax.psum_scatter(
        totals[10].astype(bf16), "dp", scatter_dimension=0, tiled=True
    ).astype(f32)
    grad_proj = lax.psum_scatter(
        totals[9]
        .reshape(head_count, LANES, model_width)[:, :HEAD_DIM]
        .reshape(head_width, model_width)
        .astype(bf16),
        "dp",
        scatter_dimension=1, tiled=True
    ).astype(f32)
    grad_qkv = lax.psum_scatter(
        totals[8]
        .reshape(model_width, 3 * head_count, LANES)[:, :, :HEAD_DIM]
        .reshape(model_width, 3, head_width)
        .astype(bf16),
        "dp",
        scatter_dimension=0,
        tiled=True,
    ).astype(f32)
    qkv_full_grad = lax.dynamic_update_slice_in_dim(
        jnp.zeros((3, model_width), f32),
        totals[2].reshape(3 * head_count, LANES)[:, :HEAD_DIM].reshape(3, head_width),
        tensor_place * head_width,
        1,
    ).reshape(3 * model_width)
    fc1_full_grad = lax.dynamic_update_slice_in_dim(
        jnp.zeros((fc1_shift.shape[0],), f32), totals[6], tensor_place * hidden_width, 0
    )
    small_out = scatter_small(
        (
            totals[0],
            totals[1],
            qkv_full_grad,
            totals[3],
            totals[4],
            totals[5],
            fc1_full_grad,
            totals[7],
        ),
        dp_count,
        tensor_count,
    )
    return (
        jnp.stack(outputs, axis=0),
        jnp.stack(token_grads, axis=0),
        small_out[0],
        small_out[1],
        grad_qkv,
        small_out[2],
        grad_proj,
        small_out[3],
        small_out[4],
        small_out[5],
        grad_fc1,
        small_out[6],
        grad_fc2,
        small_out[7],
    )


def solution(mesh):
    placed = (
        P("dp", "tensor", None),
        P("dp", None),
        P("dp", None),
        P("dp", None),
        P("dp", None),
        P(("dp", "tensor")),
        P(("dp", "tensor")),
        P("dp", None, "tensor"),
        P(("dp", "tensor")),
        P("tensor", "dp"),
        P(("dp", "tensor")),
        P(("dp", "tensor")),
        P(("dp", "tensor")),
        P("dp", "tensor"),
        P(("dp", "tensor")),
        P("tensor", "dp"),
        P(("dp", "tensor")),
        P("dp", "tensor", None),
    )
    return jax.shard_map(
        functools.partial(on_device, mesh.shape["dp"], mesh.shape["tensor"]),
        mesh=mesh,
        in_specs=placed,
        out_specs=(
            P("dp", "tensor", None),
            P("dp", "tensor", None),
            P(("dp", "tensor")),
            P(("dp", "tensor")),
            P("dp", None, "tensor"),
            P(("dp", "tensor")),
            P("tensor", "dp"),
            P(("dp", "tensor")),
            P(("dp", "tensor")),
            P(("dp", "tensor")),
            P("dp", "tensor"),
            P(("dp", "tensor")),
            P("tensor", "dp"),
            P(("dp", "tensor")),
        ),
        check_vma=False,
    )
```

```python
import functools
import math

import jax
import jax.numpy as jnp
from jax import lax
from jax.experimental import pallas as pl
from jax.experimental.pallas import tpu as pltpu
from jax.sharding import PartitionSpec as P

HEAD_DIM = 80


norm_eps = 1e-06


def layer_norm(values, gain_row, shift_row):
    center = values - jnp.mean(values, axis=-1, keepdims=True)
    spread = jnp.mean(center * center, axis=-1, keepdims=True)
    scaled = lax.rsqrt(spread + norm_eps)
    normed = center * scaled
    return (normed * gain_row + shift_row, normed, scaled)


def norm_back(grad_rows, normed, scaled, gain_row):
    grad_hat = grad_rows * gain_row
    mean_one = jnp.mean(grad_hat, axis=-1, keepdims=True)
    mean_two = jnp.mean(grad_hat * normed, axis=-1, keepdims=True)
    return scaled * (grad_hat - mean_one - normed * mean_two)


def flip_pairs(count, step):
    return [(place, place ^ step) for place in range(count)]


def relative_order(count):
    order = [0]
    step = count // 2
    while step >= 1:
        order = order + [place ^ step for place in order]
        step //= 2
    return order


def gather_rows(rows, count):
    step = count // 2
    while step >= 1:
        received = lax.ppermute(rows, "tensor", flip_pairs(count, step))
        rows = jnp.concatenate([rows, received], axis=0)
        step //= 2
    return rows


def after(values, earlier):
    return values if earlier is None else lax.optimization_barrier((values, earlier))[0]


def scatter_product(product, rows, count):
    half = rows.shape[0] // 2
    sent = product(rows[half:]).astype(jnp.bfloat16)
    received = lax.ppermute(sent, "tensor", flip_pairs(count, 1))
    total = product(rows[:half]) + received.astype(jnp.float32)
    step = 2
    while step < count:
        half = half // 2
        sent = total[half:].astype(jnp.bfloat16)
        received = lax.ppermute(sent, "tensor", flip_pairs(count, step))
        if step * 2 >= count:
            received = after(received, (yield sent))
        total = total[:half] + received.astype(jnp.float32)
        step *= 2
    yield total


def gather_small(vectors, dp_count, tensor_count):
    count = dp_count * tensor_count
    place = lax.axis_index("dp") * tensor_count + lax.axis_index("tensor")
    packed = jnp.concatenate(vectors, axis=0)
    width = packed.shape[0]
    table = lax.dynamic_update_slice_in_dim(
        jnp.zeros((count, width), packed.dtype), packed[None], place, 0
    )
    step = 1
    while step < count:
        table = table + lax.ppermute(table, ("dp", "tensor"), flip_pairs(count, step))
        step *= 2
    parts = []
    offset = 0
    for vector in vectors:
        size = vector.shape[0]
        parts.append(table[:, offset : offset + size].reshape(count * size))
        offset += size
    return parts


def scatter_small(vectors, dp_count, tensor_count):
    count = dp_count * tensor_count
    place = lax.axis_index("dp") * tensor_count + lax.axis_index("tensor")
    table = jnp.concatenate([vector.reshape(count, -1) for vector in vectors], axis=1)
    near = lax.bitwise_xor(jnp.arange(count, dtype=jnp.int32), place.astype(jnp.int32))
    table = jnp.take(table, near, axis=0)
    step = count // 2
    while step >= 1:
        received = lax.ppermute(table[step:], ("dp", "tensor"), flip_pairs(count, step))
        table = table[:step] + received
        step //= 2
    parts = []
    offset = 0
    for vector in vectors:
        size = vector.shape[0] // count
        parts.append(table[0, offset : offset + size])
        offset += size
    return parts


LANES = 128
stage_total = 7
away = 2.0 ** 66
log2_e = 1.4426950408889634


def fold_lanes(values):
    quarter_turn = HEAD_DIM // 2
    return (
        pltpu.roll(values, LANES - quarter_turn, 1),
        pltpu.roll(values, quarter_turn, 1),
    )


def nt_product(left, right):
    return lax.dot_general(
        left, right, (((1,), (1,)), ((), ())), preferred_element_type=jnp.float32
    )


def attend_forward_kernel(
    block_rows,
    score_scale,
    lin_q_ref,
    lin_k_ref,
    lin_v_ref,
    cos_ref,
    sin_low_ref,
    sin_high_ref,
    query_slot_ref,
    key_slot_ref,
    query_ref,
    key_ref,
    value_ref,
    context_ref,
    stat_ref,
):
    row_length = lin_q_ref.shape[0]

    def turned(values, slots):
        low, high = fold_lanes(values)
        return (
            values * cos_ref[...] + low * sin_low_ref[...] + high * sin_high_ref[...] + slots
        ).astype(jnp.bfloat16)

    query_ref[...] = turned(lin_q_ref[...], query_slot_ref[...])
    keys = turned(lin_k_ref[...], key_slot_ref[...])
    key_ref[...] = keys
    values = lin_v_ref[...].astype(jnp.bfloat16)
    value_ref[...] = values
    values_t = values.T
    for lower in range(0, row_length, block_rows):
        block = slice(lower, lower + block_rows)
        scores = nt_product(keys, query_ref[block, :])
        highest = jnp.max(scores, axis=0, keepdims=True)
        shifted = jnp.exp2((scores - highest) * (score_scale * log2_e))
        inverse = 1.0 / jnp.sum(shifted, axis=0, keepdims=True)
        attend = (shifted * inverse).astype(jnp.bfloat16)
        context_t = jnp.dot(values_t, attend, preferred_element_type=jnp.float32)
        context_ref[block, :] = context_t.T.astype(jnp.bfloat16)
        stat_ref[0, 0:1, block] = highest
        stat_ref[0, 1:2, block] = inverse


def attend_back_kernel(
    block_rows,
    score_scale,
    query_ref,
    key_ref,
    value_ref,
    grad_ref,
    stat_ref,
    cos_ref,
    sin_low_ref,
    sin_high_ref,
    grad_linear_ref,
    key_sum_ref,
    value_sum_ref,
):
    row_length = query_ref.shape[0]
    head = pl.program_id(0)
    heads = pl.num_programs(0)
    keys = key_ref[...]
    keys_t = keys.T
    values = value_ref[...]

    def columns(kind):
        return pl.ds(pl.multiple_of((kind * heads + head) * LANES, LANES), LANES)

    def unturned(grads, block):
        low, high = fold_lanes(grads)
        return (
            grads * cos_ref[block, :] - low * sin_low_ref[block, :] - high * sin_high_ref[block, :]
        ).astype(jnp.bfloat16)

    for lower in range(0, row_length, block_rows):
        block = slice(lower, lower + block_rows)
        queries = query_ref[block, :]
        grads = grad_ref[block, :]
        scores = nt_product(keys, queries)
        attend = (
            jnp.exp2((scores - stat_ref[0, 0:1, block]) * (score_scale * log2_e))
            * stat_ref[0, 1:2, block]
        )
        value_part = jnp.dot(
            attend.astype(jnp.bfloat16), grads, preferred_element_type=jnp.float32
        )
        attend_grad = nt_product(values, grads)
        inner = jnp.sum(attend * attend_grad, axis=0, keepdims=True)
        score_grad = (attend * (attend_grad - inner) * score_scale).astype(jnp.bfloat16)
        key_part = jnp.dot(score_grad, queries, preferred_element_type=jnp.float32)
        query_t = jnp.dot(keys_t, score_grad, preferred_element_type=jnp.float32)
        grad_linear_ref[block, columns(0)] = unturned(query_t.T, block)
        if lower == 0:
            key_sum_ref[...] = key_part
            value_sum_ref[...] = value_part
        else:
            key_sum_ref[...] += key_part
            value_sum_ref[...] += value_part
    grad_linear_ref[:, columns(1)] = unturned(key_sum_ref[...], slice(None))
    grad_linear_ref[:, columns(2)] = value_sum_ref[...].astype(jnp.bfloat16)


def head_spec(row_length, shift):
    return pl.BlockSpec((row_length, LANES), lambda head: (0, head + shift))


def whole_spec(shape):
    return pl.BlockSpec(shape, lambda head: (0,) * len(shape))


def attend_forward(linear, tables, head_count, score_scale):
    row_length = linear.shape[0]
    block_rows = min(256, row_length)
    cos_table, sin_low, sin_high, query_slots, key_slots = tables
    table = whole_spec((row_length, LANES))
    headed = jax.ShapeDtypeStruct((row_length, head_count * LANES), jnp.bfloat16)
    area = head_count * row_length * row_length
    queries, keys, values, context, stats = pl.pallas_call(
        functools.partial(attend_forward_kernel, block_rows, score_scale),
        grid=(head_count,),
        in_specs=[
            head_spec(row_length, 0),
            head_spec(row_length, head_count),
            head_spec(row_length, 2 * head_count),
        ]
        + [table] * 5,
        out_specs=[head_spec(row_length, 0)] * 4
        + [pl.BlockSpec((1, 2, row_length), lambda head: (head, 0, 0))],
        out_shape=[headed] * 4
        + [jax.ShapeDtypeStruct((head_count, 2, row_length), jnp.float32)],
        cost_estimate=pl.CostEstimate(
            flops=4 * area * LANES,
            bytes_accessed=20 * row_length * head_count * LANES,
            transcendentals=area,
        ),
        name="attend_forward",
    )(linear, linear, linear, cos_table, sin_low, sin_high, query_slots, key_slots)
    return context, (queries, keys, values, stats)


def attend_back(kept, grad_context, tables, head_count, score_scale):
    queries, keys, values, stats = kept
    row_length = queries.shape[0]
    block_rows = min(256, row_length)
    cos_table, sin_low, sin_high = tables[:3]
    table = whole_spec((row_length, LANES))
    area = head_count * row_length * row_length
    return pl.pallas_call(
        functools.partial(attend_back_kernel, block_rows, score_scale),
        grid=(head_count,),
        in_specs=[head_spec(row_length, 0)] * 4
        + [pl.BlockSpec((1, 2, row_length), lambda head: (head, 0, 0))]
        + [table] * 3,
        out_specs=whole_spec((row_length, 3 * head_count * LANES)),
        out_shape=jax.ShapeDtypeStruct((row_length, 3 * head_count * LANES), jnp.bfloat16),
        scratch_shapes=[
            pltpu.VMEM((row_length, LANES), jnp.float32),
            pltpu.VMEM((row_length, LANES), jnp.float32),
        ],
        cost_estimate=pl.CostEstimate(
            flops=10 * area * LANES,
            bytes_accessed=14 * row_length * head_count * LANES,
            transcendentals=area,
        ),
        name="attend_back",
    )(queries, keys, values, grad_context, stats, cos_table, sin_low, sin_high)


def head_tables(row_places, col_places, row_ids, row_lengths, key_places):
    quarter = HEAD_DIM // 4
    half = HEAD_DIM // 2
    slots = row_lengths.shape[0]
    freqs_base = 10000.0 ** (-(4.0 * jnp.arange(quarter, dtype=jnp.float32)) / HEAD_DIM)
    angles = jnp.concatenate(
        [
            row_places.astype(jnp.float32)[:, None] * freqs_base[None, :],
            col_places.astype(jnp.float32)[:, None] * freqs_base[None, :],
        ],
        axis=-1,
    )
    cosine = jnp.cos(angles)
    sine = jnp.sin(angles)

    def lanes(values, before):
        return jnp.pad(values, ((0, 0), (before, LANES - before - values.shape[1])))

    same = row_ids[:, None] == jnp.arange(slots, dtype=jnp.int32)[None, :]
    filled = (key_places < jnp.sum(row_lengths))[:, None]
    low_sine = lanes(sine, 0)
    high_sine = lanes(sine, half)
    return (
        lanes(jnp.concatenate([cosine, cosine], axis=-1), 0),
        -low_sine,
        high_sine,
        lanes(same.astype(jnp.float32), HEAD_DIM),
        lanes(jnp.where(same & filled, 0.0, -away), HEAD_DIM),
    )


def dot_nn(left, right):
    return jnp.dot(left, right, preferred_element_type=jnp.float32)


def dot_nt(left, right):
    return jnp.einsum("sk,nk->sn", left, right, preferred_element_type=jnp.float32)


def dot_tn(left, right):
    return jnp.einsum("sm,sn->mn", left, right, preferred_element_type=jnp.float32)


def on_device(
    dp_count,
    tensor_count,
    tokens,
    pic_ids,
    pos_rows,
    pos_cols,
    lengths,
    ln1_gain,
    ln1_bias,
    qkv_weight,
    qkv_bias,
    proj_weight,
    proj_bias,
    ln2_gain,
    ln2_bias,
    fc1_weight,
    fc1_bias,
    fc2_weight,
    fc2_bias,
    cotangent,
):
    row_total = tokens.shape[0]
    local_rows = tokens.shape[1]
    model_width = tokens.shape[2]
    row_length = pic_ids.shape[1]
    head_width = qkv_weight.shape[2]
    hidden_width = fc1_weight.shape[1]
    head_count = head_width // HEAD_DIM
    score_scale = 1.0 / math.sqrt(HEAD_DIM)
    tensor_place = lax.axis_index("tensor")
    f32 = jnp.float32
    bf16 = jnp.bfloat16
    order = jnp.array(relative_order(tensor_count), jnp.int32)
    block_ids = lax.bitwise_xor(order, tensor_place.astype(jnp.int32))
    all_places = (
        block_ids[:, None] * local_rows + jnp.arange(local_rows, dtype=jnp.int32)[None, :]
    ).reshape(row_length)

    def near_order(values):
        return jnp.take(values.reshape(tensor_count, local_rows), block_ids, axis=0).reshape(
            row_length
        )

    local_places = all_places[:local_rows]
    vectors = gather_small(
        (ln1_gain, ln1_bias, qkv_bias, proj_bias, ln2_gain, ln2_bias, fc1_bias, fc2_bias),
        dp_count,
        tensor_count,
    )
    gain_one, shift_one, qkv_shift, proj_shift, gain_two, shift_two, fc1_shift, fc2_shift = [
        vector_part.astype(f32) for vector_part in vectors
    ]
    qkv_local_shift = lax.dynamic_slice_in_dim(
        qkv_shift.reshape(3, model_width), tensor_place * head_width, head_width, 1
    ).reshape(3 * head_width)
    fc1_local_shift = lax.dynamic_slice_in_dim(
        fc1_shift, tensor_place * hidden_width, hidden_width, 0
    )
    w_qkv = lax.all_gather(qkv_weight, "dp", axis=0, tiled=True)
    w_proj = lax.all_gather(proj_weight, "dp", axis=1, tiled=True)
    w_fc1 = lax.all_gather(fc1_weight, "dp", axis=0, tiled=True)
    w_fc2 = lax.all_gather(fc2_weight, "dp", axis=1, tiled=True)
    spare = LANES - HEAD_DIM
    w_qkv_flat = jnp.pad(
        w_qkv.reshape(model_width, 3 * head_count, HEAD_DIM), ((0, 0), (0, 0), (0, spare))
    ).reshape(model_width, 3 * head_count * LANES)
    w_proj = jnp.pad(
        w_proj.reshape(head_count, HEAD_DIM, model_width), ((0, 0), (0, spare), (0, 0))
    ).reshape(head_count * LANES, model_width)
    qkv_local_shift = jnp.pad(
        qkv_local_shift.reshape(3 * head_count, HEAD_DIM), ((0, 0), (0, spare))
    ).reshape(3 * head_count * LANES)

    def row_stages(row):
        tokens_row = tokens[row].astype(f32)
        tables = all_tables[row]
        pad_rows = (local_places < jnp.sum(lengths[row])).astype(f32)[:, None]
        grad_out = pad_rows * cotangent[row].astype(f32)
        normed_one, hat_one, scale_one = layer_norm(tokens_row, gain_one, shift_one)
        normed_one = normed_one.astype(bf16)
        grad_branch = grad_out.astype(bf16)
        lowered_one = gather_rows(normed_one, tensor_count)
        earlier = yield normed_one

        lowered_one = after(lowered_one, earlier)
        linear = dot_nn(lowered_one, w_qkv_flat) + qkv_local_shift
        context_bf, kept = attend_forward(linear, tables, head_count, score_scale)
        attn_scatter = scatter_product(
            lambda part: dot_nn(part, w_proj), context_bf, tensor_count
        )
        earlier = yield next(attn_scatter)

        attn_branch = attn_scatter.send(earlier)
        hidden_row = tokens_row + attn_branch + proj_shift
        normed_two, hat_two, scale_two = layer_norm(hidden_row, gain_two, shift_two)
        normed_two = normed_two.astype(bf16)
        lowered_two = gather_rows(normed_two, tensor_count)
        grad_branch = gather_rows(after(grad_branch, normed_one), tensor_count)
        earlier = yield normed_two

        lowered_two = after(lowered_two, earlier)
        upward = dot_nn(lowered_two, w_fc1) + fc1_local_shift
        sigmoid_up = jax.nn.sigmoid(1.702 * upward)
        activated = (upward * sigmoid_up).astype(bf16)
        grad_up = (
            dot_nt(grad_branch, w_fc2)
            * (sigmoid_up + 1.702 * upward * sigmoid_up * (1.0 - sigmoid_up))
        ).astype(bf16)
        hidden_scatter = scatter_product(
            lambda part: dot_nt(part, w_fc1), grad_up, tensor_count
        )
        hidden_sent = next(hidden_scatter)
        branch_scatter = scatter_product(
            lambda part: dot_nn(part, w_fc2), after(activated, hidden_sent), tensor_count
        )
        branch_sent = next(branch_scatter)
        earlier = yield branch_sent

        grad_normed_two = hidden_scatter.send(earlier)
        grad_hidden = grad_out + norm_back(grad_normed_two, hat_two, scale_two, gain_two)
        grad_hidden_bf = grad_hidden.astype(bf16)
        grad_attn = gather_rows(grad_hidden_bf, tensor_count)
        earlier = yield grad_hidden_bf

        grad_attn = after(grad_attn, earlier)
        grad_context = dot_nt(grad_attn, w_proj).astype(bf16)
        grad_linear = attend_back(kept, grad_context, tables, head_count, score_scale)
        first_scatter = scatter_product(
            lambda part: dot_nt(part, w_qkv_flat), grad_linear, tensor_count
        )
        earlier = yield next(first_scatter)

        branch = branch_scatter.send(None)
        output = (pad_rows * (hidden_row + branch + fc2_shift)).astype(bf16)
        grad_normed_one = first_scatter.send(earlier)
        token_grad = (
            grad_hidden + norm_back(grad_normed_one, hat_one, scale_one, gain_one)
        ).astype(bf16)
        yield (
            output,
            token_grad,
            (
                jnp.sum(grad_normed_one * hat_one, axis=0),
                jnp.sum(grad_normed_one, axis=0),
                jnp.sum(grad_linear.astype(f32), axis=0),
                jnp.sum(grad_hidden, axis=0),
                jnp.sum(grad_normed_two * hat_two, axis=0),
                jnp.sum(grad_normed_two, axis=0),
                jnp.sum(grad_up.astype(f32), axis=0),
                jnp.sum(grad_out, axis=0),
                dot_tn(lowered_one, grad_linear),
                dot_tn(context_bf, grad_attn),
                dot_tn(lowered_two, grad_up),
                dot_tn(activated, grad_branch),
            ),
        )

    all_tables = [
        head_tables(
            near_order(pos_rows[row]),
            near_order(pos_cols[row]),
            near_order(pic_ids[row]),
            lengths[row],
            all_places,
        )
        for row in range(row_total)
    ]
    w_qkv_flat = after(w_qkv_flat, all_tables)
    stages = [row_stages(row) for row in range(row_total)]
    tokens_out = [next(stage) for stage in stages]
    for _ in range(stage_total - 1):
        for row in range(row_total):
            tokens_out[row] = stages[row].send(tokens_out[row - 1])
    outputs = [parts[0] for parts in tokens_out]
    token_grads = [parts[1] for parts in tokens_out]
    totals = tokens_out[0][2]
    for parts in tokens_out[1:]:
        totals = tuple(first + second for first, second in zip(totals, parts[2]))

    grad_fc2 = lax.psum_scatter(
        totals[11].astype(bf16), "dp", scatter_dimension=1, tiled=True
    ).astype(f32)
    grad_fc1 = lax.psum_scatter(
        totals[10].astype(bf16), "dp", scatter_dimension=0, tiled=True
    ).astype(f32)
    grad_proj = lax.psum_scatter(
        totals[9]
        .reshape(head_count, LANES, model_width)[:, :HEAD_DIM]
        .reshape(head_width, model_width)
        .astype(bf16),
        "dp",
        scatter_dimension=1, tiled=True
    ).astype(f32)
    grad_qkv = lax.psum_scatter(
        totals[8]
        .reshape(model_width, 3 * head_count, LANES)[:, :, :HEAD_DIM]
        .reshape(model_width, 3, head_width)
        .astype(bf16),
        "dp",
        scatter_dimension=0,
        tiled=True,
    ).astype(f32)
    qkv_full_grad = lax.dynamic_update_slice_in_dim(
        jnp.zeros((3, model_width), f32),
        totals[2].reshape(3 * head_count, LANES)[:, :HEAD_DIM].reshape(3, head_width),
        tensor_place * head_width,
        1,
    ).reshape(3 * model_width)
    fc1_full_grad = lax.dynamic_update_slice_in_dim(
        jnp.zeros((fc1_shift.shape[0],), f32), totals[6], tensor_place * hidden_width, 0
    )
    small_out = scatter_small(
        (
            totals[0],
            totals[1],
            qkv_full_grad,
            totals[3],
            totals[4],
            totals[5],
            fc1_full_grad,
            totals[7],
        ),
        dp_count,
        tensor_count,
    )
    return (
        jnp.stack(outputs, axis=0),
        jnp.stack(token_grads, axis=0),
        small_out[0],
        small_out[1],
        grad_qkv,
        small_out[2],
        grad_proj,
        small_out[3],
        small_out[4],
        small_out[5],
        grad_fc1,
        small_out[6],
        grad_fc2,
        small_out[7],
    )


def solution(mesh):
    placed = (
        P("dp", "tensor", None),
        P("dp", None),
        P("dp", None),
        P("dp", None),
        P("dp", None),
        P(("dp", "tensor")),
        P(("dp", "tensor")),
        P("dp", None, "tensor"),
        P(("dp", "tensor")),
        P("tensor", "dp"),
        P(("dp", "tensor")),
        P(("dp", "tensor")),
        P(("dp", "tensor")),
        P("dp", "tensor"),
        P(("dp", "tensor")),
        P("tensor", "dp"),
        P(("dp", "tensor")),
        P("dp", "tensor", None),
    )
    return jax.shard_map(
        functools.partial(on_device, mesh.shape["dp"], mesh.shape["tensor"]),
        mesh=mesh,
        in_specs=placed,
        out_specs=(
            P("dp", "tensor", None),
            P("dp", "tensor", None),
            P(("dp", "tensor")),
            P(("dp", "tensor")),
            P("dp", None, "tensor"),
            P(("dp", "tensor")),
            P("tensor", "dp"),
            P(("dp", "tensor")),
            P(("dp", "tensor")),
            P(("dp", "tensor")),
            P("dp", "tensor"),
            P(("dp", "tensor")),
            P("tensor", "dp"),
            P(("dp", "tensor")),
        ),
        check_vma=False,
    )
```
